256 devices in a mesh: patch: 32 (over z, y), seq: 4 (over x), req: 2 (over core).
Axes of the slice: x: 4, y: 4, z: 8, core: 2. Of those that a mesh axis runs over, the one named last changes fastest.
Arguments:
- query: bfloat16 [4, 64, 3584], P(None, ('patch', 'req')), may hold values from -20 to 20
- text_cache: bfloat16 [4, 64, 3072, 1024], P(None, ('patch', 'req'), 'seq'), may hold values from -6 to 6
- text_len: int32 [64], P(('patch', 'req')), may hold values from 0 to 3072
- image_rows: bfloat16 [4, 65536, 1024], P(None, ('patch', 'seq', 'req')), may hold values from -6 to 6
- patch_map: int32 [65536], P(('patch', 'seq', 'req')), may hold values from 0 to 63, as said below
- image_places: int32 [65536], P(('patch', 'seq', 'req')), may hold values from 0 to 1023, as said below
Outputs:
- attended: bfloat16 [4, 64, 3584], P(None, ('patch', 'req'), 'seq')
- image_cache: bfloat16 [4, 64, 1024, 1024], P(None, ('patch', 'req'), 'seq')
The draws below stay inside these ranges and needn't reach their ends.
Inputs may be any that keep to these rules, and one draw needn't show every extreme that they name: `patch_map`: each aligned block of 256 rows (the rows of one prefill device) holds exactly 4 rows of every request. `image_places`: together with patch_map every pair of request and position occurs exactly once. The rows of a device whose seq index is s have positions from s * 256 to (s + 1) * 256 - 1.
All inputs are finite; a program needn't handle non-finite values.
Results may differ from the reference program's by a relative error of at most 0.0026.
Values may be sent and summed in bfloat16 or wider, within the bound.
A program may use at most 64 MiB of HBM per device.

```python
import math
import jax
import jax.numpy as jnp
from jax import lax

HEADS = 28
KV_HEADS = 4
HEAD_DIM = 128
LAYERS = 4
IMG = 1024
TXT = 3072
REQUESTS = 64
KVW = 512
N_PATCH = 32
N_SEQ = 4
N_REQ = 2


def layout_rows(key):
    groups = N_PATCH * N_REQ
    band_size = IMG // N_SEQ
    per_source = band_size // groups
    device_count = N_PATCH * N_SEQ * N_REQ
    pair_keys = jax.random.split(jax.random.fold_in(key, 7001), N_SEQ * REQUESTS)
    shuffled = jax.vmap(lambda piece: jax.random.permutation(piece, band_size))(pair_keys)
    shuffled = shuffled.astype(jnp.int32).reshape(N_SEQ, REQUESTS, N_PATCH, N_REQ, per_source)
    band_start = (jnp.arange(N_SEQ, dtype=jnp.int32) * band_size)[:, None, None, None, None]
    places = shuffled + band_start
    owners = jnp.broadcast_to(jnp.arange(REQUESTS, dtype=jnp.int32)[None, :, None, None, None], places.shape)
    places = jnp.transpose(places, (2, 0, 3, 1, 4)).reshape(device_count, REQUESTS * per_source)
    owners = jnp.transpose(owners, (2, 0, 3, 1, 4)).reshape(device_count, REQUESTS * per_source)
    row_keys = jax.random.split(jax.random.fold_in(key, 7002), device_count)
    mixing = jax.vmap(lambda piece: jax.random.permutation(piece, REQUESTS * per_source))(row_keys)
    mixing = mixing.astype(jnp.int32)
    places = jnp.take_along_axis(places, mixing, axis=1).reshape(-1)
    owners = jnp.take_along_axis(owners, mixing, axis=1).reshape(-1)
    return (owners, places)


def draw_patch_map(key, part):
    return layout_rows(key)[0]


def draw_image_places(key, part):
    return layout_rows(key)[1]


def draw_query(key, part):
    shape = (LAYERS, REQUESTS, HEADS * HEAD_DIM)
    noise_key = jax.random.fold_in(key, 7004)
    values = jnp.clip(2.5 * jax.random.normal(noise_key, shape, jnp.float32), -12.0, 12.0)
    return values.astype(jnp.bfloat16)


def draw_image_rows(key, part):
    shape = (LAYERS, REQUESTS * IMG, 2 * KV_HEADS * HEAD_DIM)
    noise_key = jax.random.fold_in(key, 7005)
    values = jnp.clip(jax.random.normal(noise_key, shape, jnp.float32), -6.0, 6.0)
    return values.astype(jnp.bfloat16)


def place_ends(values, own_key, least, top_value):
    index_at = [jax.random.randint(jax.random.fold_in(own_key, axis), (), 0, length) for axis, length in enumerate(values.shape)]
    longest = values.shape.index(max(values.shape))
    neighbour = index_at[:longest] + [(index_at[longest] + 1) % values.shape[longest]] + index_at[longest + 1:]
    return values.at[tuple(index_at)].set(least).at[tuple(neighbour)].set(top_value)


def block_levels(rng, shape, cuts, low, largest):
    loudness, own = 1.0, jax.random.fold_in(rng, 6)
    for position, shards_of in cuts:
        steps = jnp.exp(jax.random.uniform(jax.random.fold_in(own, position), (shards_of,), jnp.float32, low / len(cuts), largest / len(cuts)))
        loudness = loudness * jnp.repeat(steps, shape[position] // shards_of).reshape([-1 if axis == position else 1 for axis in range(len(shape))])
    return loudness


def bell_draw(rng, dims, deviation, most, cuts=(), kind=jnp.bfloat16):
    result = deviation * jax.random.normal(rng, dims, jnp.float32)
    if cuts:
        result = result * block_levels(rng, dims, cuts, -0.22, 0.18)
    return jnp.clip(result, -most, most).astype(kind)


def setup_inputs(seed: int = 0) -> dict:
    seeds = jax.random.split(jax.random.key(seed), 7)
    return {
        "query": draw_query(jax.random.fold_in(seeds[6], 71), 0),
        "text_cache": bell_draw(seeds[1], (LAYERS, REQUESTS, TXT, 2 * KVW), 1.0, 6.0, ((1, 64), (2, 4))),
        "text_len": place_ends(jax.random.randint(seeds[2], (REQUESTS,), 0, TXT + 1), jax.random.fold_in(seeds[2], 1), 0, TXT).astype(jnp.int32),
        "image_rows": draw_image_rows(jax.random.fold_in(seeds[6], 71), 0),
        "patch_map": draw_patch_map(jax.random.fold_in(seeds[6], 71), 0),
        "image_places": draw_image_places(jax.random.fold_in(seeds[6], 71), 0),
    }


def attend_one(query_row, image_block, text_block, length):
    kv_width = KV_HEADS * HEAD_DIM
    group = HEADS // KV_HEADS
    band_size = IMG // N_SEQ
    text_band = TXT // N_SEQ
    image_banded = image_block.reshape(N_SEQ, band_size, 2 * kv_width)
    text_banded = text_block.reshape(N_SEQ, text_band, 2 * kv_width)
    keys_all = jnp.concatenate([image_banded, text_banded], axis=1)
    width = band_size + text_band
    keys = keys_all[:, :, :kv_width].reshape(N_SEQ, width, KV_HEADS, HEAD_DIM).astype(jnp.float32)
    values = keys_all[:, :, kv_width:].reshape(N_SEQ, width, KV_HEADS, HEAD_DIM).astype(jnp.float32)
    queries = query_row.reshape(KV_HEADS, group, HEAD_DIM).astype(jnp.float32)
    scores = jnp.einsum('kgd,stkd->skgt', queries, keys) * (1.0 / math.sqrt(HEAD_DIM))
    inner = jnp.arange(width, dtype=jnp.int32)
    bands = jnp.arange(N_SEQ, dtype=jnp.int32)
    text_pos = bands[:, None] * text_band + inner[None, :] - band_size
    used = (inner[None, :] < band_size) | (text_pos < length)
    scores = jnp.where(used[:, None, None, :], scores, -jnp.inf)
    band_top = lax.optimization_barrier(jnp.max(scores, axis=-1, keepdims=True))
    weights = jnp.exp(scores - band_top)
    band_total = lax.optimization_barrier(jnp.sum(weights, axis=-1))
    rounded = lax.optimization_barrier(weights.astype(jnp.bfloat16)).astype(jnp.float32)
    band_sum = jnp.einsum('skgt,stkd->skgd', rounded, values)
    band_top = band_top[..., 0]
    top = lax.optimization_barrier(jnp.max(band_top, axis=0, keepdims=True))
    factor = jnp.exp(band_top - top)
    total = lax.optimization_barrier(jnp.sum(factor * band_total, axis=0))
    summed = lax.optimization_barrier(jnp.sum(factor[..., None] * band_sum, axis=0))
    return (summed / total[..., None]).reshape(HEADS * HEAD_DIM).astype(jnp.bfloat16)

def attend_packed(packed):
    return attend_one(packed[0], packed[1], packed[2], packed[3])

def reference(query, text_cache, text_len, image_rows, patch_map, image_places):
    order = jnp.argsort(patch_map * IMG + image_places)
    image_cache = jnp.take(image_rows, order, axis=1).reshape(LAYERS, REQUESTS, IMG, image_rows.shape[2])

    def per_layer(packed):
        return lax.map(attend_packed, (packed[0], packed[1], packed[2], text_len))
    attended = lax.map(per_layer, (query, image_cache, text_cache))
    return (attended, image_cache)
```

```python
import functools
import math

import jax
import jax.numpy as jnp
from jax import lax
from jax.experimental import pallas as pl
from jax.experimental.pallas import tpu as pltpu
from jax.sharding import PartitionSpec as P

HEADS = 28
KV_HEADS = 4
HEAD_DIM = 128
GROUP = HEADS // KV_HEADS
PAD = 8
MESH = pl.DeviceIdType.MESH
BF16 = jnp.bfloat16
F32 = jnp.float32
CHUNKS = ((0, 512), (512, 256), (768, 256))


def kernel(
    dims,
    pm_hbm, pos_hbm, len_ref, query_hbm, text_hbm, rows_hbm,
    att_ref, cache_ref,
    pm_ref, pos_ref, query_ref, text_ref, rows_ref,
    sort_ref, send_ref, got_ref, place_ref,
    place_send, place_got, q_ref, score_ref, weight_ref, acc_ref, stat_ref, acc_got, stat_got,
    in_sems, send_sem, recv_sems, place_sem, xsend_sem, xstat_sem, xacc_sem,
):
    patches, seqs, reqs, layers, slot, band, text_dev = dims
    peers = patches * reqs
    msg = layers * slot
    total_rows = layers * band
    patch, seq, req = (lax.axis_index(n) for n in ("patch", "seq", "req"))
    me = patch * reqs + req
    scale = 1.0 / math.sqrt(HEAD_DIM)
    n_chunks = len(CHUNKS)

    def peer(step):
        other = lax.rem(me + step, peers)
        return other, {"patch": other // reqs, "req": lax.rem(other, reqs)}

    loads = [
        pltpu.make_async_copy(src, dst, in_sems.at[i])
        for i, (src, dst) in enumerate(
            (
                (pm_hbm, pm_ref),
                (pos_hbm, pos_ref),
                (rows_hbm, rows_ref),
                (query_hbm, query_ref),
                (text_hbm, text_ref),
            )
        )
    ]
    loads[0].start()
    loads[1].start()
    loads[2].start()

    barrier = pltpu.get_barrier_semaphore()

    def greet(step, carry):
        _, device = peer(step)
        pl.semaphore_signal(barrier, inc=1, device_id=device, device_id_type=MESH)
        return carry

    lax.fori_loop(1, peers, greet, 0)
    for step in range(1, seqs):
        pl.semaphore_signal(
            barrier, inc=1, device_id={"seq": lax.rem(seq + step, seqs)}, device_id_type=MESH
        )
    loads[3].start()
    loads[4].start()

    loads[0].wait()
    loads[1].wait()
    owner = pm_ref[...]
    member = lax.broadcasted_iota(jnp.int32, (peers, band), 0) == owner
    member_f = member.astype(F32)
    before = lax.broadcasted_iota(jnp.int32, (band, band), 0) < lax.broadcasted_iota(
        jnp.int32, (band, band), 1
    )
    counts = jnp.dot(
        member_f.astype(BF16), before.astype(F32).astype(BF16), preferred_element_type=F32
    )
    rank = jnp.sum(member_f * counts, axis=0, keepdims=True)
    target = owner.astype(F32) * msg + rank
    line = lax.broadcasted_iota(jnp.int32, (total_rows, band), 0).astype(F32)
    for l in range(layers):
        sort_ref[:, l * band : (l + 1) * band] = (
            (line == target + float(l * slot)).astype(F32).astype(BF16)
        )

    local = pos_ref[...].astype(F32) - (seq * band).astype(F32)
    lane = lax.broadcasted_iota(jnp.int32, (peers, 128), 1)
    spread = ((lane // slot) % layers * band).astype(F32)
    for k in range(slot):
        mine = jnp.where(member & (counts == float(k)), local, 0.0)
        spread = spread + jnp.where(lane % slot == k, jnp.sum(mine, axis=1, keepdims=True), 0.0)
    place_send[...] = spread.reshape(peers, 1, 128)

    loads[2].wait()

    def sort_chunk(c):
        start, width = CHUNKS[c]
        for j in range(start, start + width, 256):
            def rows_of(i, carry):
                lines = pl.ds(pl.multiple_of(i * 256, 256), 256)
                send_ref[lines, j : j + 256] = jnp.dot(
                    sort_ref[lines, :], rows_ref[:, j : j + 256], preferred_element_type=F32
                ).astype(BF16)
                return carry
            lax.fori_loop(0, total_rows // 256, rows_of, 0)

    def block(ref, index, c):
        start, width = CHUNKS[c]
        return ref.at[pl.ds(pl.multiple_of(index * msg, msg), msg), pl.ds(start, width)]

    def send_chunk(c):
        def send(step, carry):
            other, device = peer(step)
            pltpu.make_async_remote_copy(
                src_ref=block(send_ref, other, c),
                dst_ref=block(got_ref, me, c),
                send_sem=send_sem,
                recv_sem=recv_sems.at[c],
                device_id=device,
                device_id_type=MESH,
            ).start()
            return carry
        lax.fori_loop(1, peers, send, 0)

    sort_chunk(0)
    pl.semaphore_wait(barrier, peers - 1 + seqs - 1)

    def send_place(step, carry):
        other, device = peer(step)
        pltpu.make_async_remote_copy(
            src_ref=place_send.at[other],
            dst_ref=place_got.at[me],
            send_sem=send_sem,
            recv_sem=place_sem,
            device_id=device,
            device_id_type=MESH,
        ).start()
        return carry

    lax.fori_loop(1, peers, send_place, 0)
    send_chunk(0)
    for c in range(1, n_chunks):
        sort_chunk(c)
        send_chunk(c)
    own = pl.ds(pl.multiple_of(me * msg, msg), msg)
    got_ref[own, :] = send_ref[own, :]
    place_got[pl.ds(me, 1)] = place_send[pl.ds(me, 1)]

    loads[3].wait()
    q_ref[...] = jnp.zeros_like(q_ref)
    for l in range(layers):
        whole = query_ref[l].astype(F32)
        for h in range(HEADS):
            g, k = divmod(h, GROUP)
            q_ref[g, l * PAD + k : l * PAD + k + 1, :] = whole[:, h * HEAD_DIM : (h + 1) * HEAD_DIM]

    loads[4].wait()
    length = len_ref[0]
    text_at = lax.broadcasted_iota(jnp.int32, (PAD, text_dev), 1) + seq * text_dev
    used = text_at < length

    def dot_t(a, b):
        return lax.dot_general(a, b, (((1,), (1,)), ((), ())), preferred_element_type=F32)

    for g in range(KV_HEADS):
        keys = slice(g * HEAD_DIM, (g + 1) * HEAD_DIM)
        for l in range(layers):
            lines = slice(l * PAD, (l + 1) * PAD)
            raw = dot_t(q_ref[g, lines, :].astype(BF16), text_ref[l, :, keys]) * scale
            score_ref[g, lines, :] = jnp.where(used, raw, -jnp.inf)

    def wait_all(sem, ref):
        pltpu.make_async_copy(ref, ref, sem).wait()

    wait_all(place_sem, place_got.at[pl.ds(0, peers - 1)])
    per_tile = 128 // msg
    first = lax.broadcasted_iota(jnp.int32, (per_tile, 128), 0)
    which = lax.broadcasted_iota(jnp.int32, (per_tile, 128), 1) // msg
    cache_line = lax.broadcasted_iota(jnp.int32, (total_rows, 128), 0).astype(F32)
    for b in range(peers // per_tile):
        tile = place_got[b * per_tile : (b + 1) * per_tile].reshape(per_tile, 128)
        to = jnp.sum(jnp.where(first == which, tile, 0.0), axis=0, keepdims=True)
        place_ref[:, b * 128 : (b + 1) * 128] = (cache_line == to).astype(F32).astype(BF16)

    def place_chunk(c):
        start, width = CHUNKS[c]
        for j in range(start, start + width, 256):
            def rows_of(i, carry):
                lines = pl.ds(pl.multiple_of(i * 256, 256), 256)
                cache_ref[lines, j : j + 256] = jnp.dot(
                    place_ref[lines, :], got_ref[:, j : j + 256], preferred_element_type=F32
                ).astype(BF16)
                return carry
            lax.fori_loop(0, total_rows // 256, rows_of, 0)

    def wait_chunk(c):
        start, width = CHUNKS[c]
        wait_all(
            recv_sems.at[c], got_ref.at[pl.ds(0, (peers - 1) * msg), pl.ds(start, width)]
        )

    def exchange(src_ref, dst_ref, g, sem):
        @pl.when(seq != g)
        def _():
            pltpu.make_async_remote_copy(
                src_ref=src_ref.at[g],
                dst_ref=dst_ref.at[seq],
                send_sem=xsend_sem,
                recv_sem=sem,
                device_id={"seq": g},
                device_id_type=MESH,
            ).start()

    wait_chunk(0)
    same_layer = (
        lax.broadcasted_iota(jnp.int32, (layers * PAD, total_rows), 1) // slot
    ) % layers == lax.broadcasted_iota(jnp.int32, (layers * PAD, total_rows), 0) // PAD
    half = lax.broadcasted_iota(jnp.int32, (layers * PAD, 128), 1) < 64
    for g in range(KV_HEADS):
        keys = slice(g * HEAD_DIM, (g + 1) * HEAD_DIM)
        vals = slice((KV_HEADS + g) * HEAD_DIM, (KV_HEADS + g + 1) * HEAD_DIM)
        raw = dot_t(q_ref[g].astype(BF16), got_ref[:, keys]) * scale
        image = jnp.where(same_layer, raw, -jnp.inf)
        text = score_ref[g]
        top = jnp.maximum(
            jnp.max(image, axis=1, keepdims=True), jnp.max(text, axis=1, keepdims=True)
        )
        image_w = jnp.exp(image - top)
        text_w = jnp.exp(text - top)
        total = jnp.sum(image_w, axis=1, keepdims=True) + jnp.sum(text_w, axis=1, keepdims=True)
        weight_ref[g] = image_w.astype(BF16)
        stat_ref[g] = jnp.where(half, top, total)
        for l in range(layers):
            lines = slice(l * PAD, (l + 1) * PAD)
            acc_ref[g, lines, :] = jnp.dot(
                text_w[lines].astype(BF16), text_ref[l, :, vals], preferred_element_type=F32
            )
    for g in range(KV_HEADS):
        exchange(stat_ref, stat_got, g, xstat_sem)
    stat_got[pl.ds(seq, 1)] = stat_ref[pl.ds(seq, 1)]
    place_chunk(0)

    for c in range(1, n_chunks):
        wait_chunk(c)
        start, width = CHUNKS[c]
        heads = range(start // HEAD_DIM - KV_HEADS, (start + width) // HEAD_DIM - KV_HEADS)
        for g in heads:
            vals = slice((KV_HEADS + g) * HEAD_DIM, (KV_HEADS + g + 1) * HEAD_DIM)
            acc_ref[g] = acc_ref[g] + jnp.dot(
                weight_ref[g], got_ref[:, vals], preferred_element_type=F32
            )
        for g in heads:
            exchange(acc_ref, acc_got, g, xacc_sem)
        place_chunk(c)
    acc_got[pl.ds(seq, 1)] = acc_ref[pl.ds(seq, 1)]

    wait_all(xstat_sem, stat_got.at[pl.ds(0, seqs - 1)])
    tops = [stat_got[b][:, 0:1] for b in range(seqs)]
    totals = [stat_got[b][:, 64:65] for b in range(seqs)]
    top = functools.reduce(jnp.maximum, tops)
    factors = [jnp.exp(t - top) for t in tops]
    total = sum(f * t for f, t in zip(factors, totals))
    wait_all(xacc_sem, acc_got.at[pl.ds(0, seqs - 1)])
    summed = sum(f * acc_got[b] for b, f in enumerate(factors))
    result = summed / total
    for l in range(layers):
        for k in range(GROUP):
            att_ref[l, :, k * HEAD_DIM : (k + 1) * HEAD_DIM] = result[
                l * PAD + k : l * PAD + k + 1, :
            ].astype(BF16)

    for c in range(n_chunks):
        start, width = CHUNKS[c]
        wait_all(send_sem, got_ref.at[pl.ds(0, (peers - 1) * msg), pl.ds(start, width)])
    wait_all(send_sem, place_got.at[pl.ds(0, peers - 1)])
    wait_all(xsend_sem, stat_got.at[pl.ds(0, seqs - 1)])
    wait_all(xsend_sem, acc_got.at[pl.ds(0, seqs - 1)])


def body(query, text_cache, text_len, image_rows, patch_map, image_places):
    layers = query.shape[0]
    text_dev = text_cache.shape[2]
    width = text_cache.shape[3]
    band = image_rows.shape[1]
    patches, seqs, reqs = (lax.axis_size(n) for n in ("patch", "seq", "req"))
    peers = patches * reqs
    slot = band // peers
    rows = layers * band
    heads = layers * PAD
    dims = (patches, seqs, reqs, layers, slot, band, text_dev)
    hbm = pl.BlockSpec(memory_space=pl.ANY)
    vmem = pl.BlockSpec(memory_space=pltpu.VMEM)
    attended, cache = pl.pallas_call(
        functools.partial(kernel, dims),
        name="reshard_attend",
        out_shape=(
            jax.ShapeDtypeStruct((layers, 1, GROUP * HEAD_DIM), BF16),
            jax.ShapeDtypeStruct((rows, width), BF16),
        ),
        in_specs=[hbm, hbm, pl.BlockSpec(memory_space=pltpu.SMEM), hbm, hbm, hbm],
        out_specs=(vmem, vmem),
        scratch_shapes=[
            pltpu.VMEM((1, band), jnp.int32),
            pltpu.VMEM((1, band), jnp.int32),
            pltpu.VMEM(query.shape, BF16),
            pltpu.VMEM((layers, text_dev, width), BF16),
            pltpu.VMEM((rows, width), BF16),
            pltpu.VMEM((rows, rows), BF16),
            pltpu.VMEM((rows, width), BF16),
            pltpu.VMEM((rows, width), BF16),
            pltpu.VMEM((rows, rows), BF16),
            pltpu.VMEM((peers, 1, 128), F32),
            pltpu.VMEM((peers, 1, 128), F32),
            pltpu.VMEM((KV_HEADS, heads, HEAD_DIM), F32),
            pltpu.VMEM((KV_HEADS, heads, text_dev), F32),
            pltpu.VMEM((KV_HEADS, heads, rows), BF16),
            pltpu.VMEM((KV_HEADS, heads, HEAD_DIM), F32),
            pltpu.VMEM((KV_HEADS, heads, HEAD_DIM), F32),
            pltpu.VMEM((seqs, heads, HEAD_DIM), F32),
            pltpu.VMEM((seqs, heads, HEAD_DIM), F32),
            pltpu.SemaphoreType.DMA((5,)),
            pltpu.SemaphoreType.DMA,
            pltpu.SemaphoreType.DMA((len(CHUNKS),)),
            pltpu.SemaphoreType.DMA,
            pltpu.SemaphoreType.DMA,
            pltpu.SemaphoreType.DMA,
            pltpu.SemaphoreType.DMA,
        ],
        compiler_params=pltpu.CompilerParams(
            collective_id=0, has_side_effects=True, vmem_limit_bytes=48 * 1024 * 1024
        ),
    )(
        patch_map.reshape(1, band),
        image_places.reshape(1, band),
        text_len,
        query,
        text_cache.reshape(layers, text_dev, width),
        image_rows.reshape(rows, width),
    )
    return attended, cache.reshape(layers, 1, band, width)


def solution(mesh):
    return jax.shard_map(
        body,
        mesh=mesh,
        in_specs=(
            P(None, ("patch", "req"), None),
            P(None, ("patch", "req"), "seq", None),
            P(("patch", "req")),
            P(None, ("patch", "seq", "req"), None),
            P(("patch", "seq", "req")),
            P(("patch", "seq", "req")),
        ),
        out_specs=(P(None, ("patch", "req"), "seq"), P(None, ("patch", "req"), "seq", None)),
        check_vma=False,
    )
```

```python
import functools
import math

import jax
import jax.numpy as jnp
from jax import lax
from jax.experimental import pallas as pl
from jax.experimental.pallas import tpu as pltpu
from jax.sharding import PartitionSpec as P

HEADS = 28
KV_HEADS = 4
HEAD_DIM = 128
GROUP = HEADS // KV_HEADS
PAD = 8
MESH = pl.DeviceIdType.MESH
BF16 = jnp.bfloat16
F32 = jnp.float32
CHUNKS = ((0, 512), (512, 256), (768, 256))


def kernel(
    dims,
    len_ref, pm_hbm, pos_hbm, query_hbm, text_hbm, rows_hbm,
    att_ref, cache_ref,
    pm_ref, pos_ref, query_ref, text_ref, rows_ref,
    sort_ref, send_ref, got_ref, place_ref,
    place_send, place_got, q_ref, score_ref, weight_ref, acc_ref, stat_ref, acc_got, stat_got,
    in_sems, send_sem, recv_sems, place_sem, xsend_sem, xstat_sem, xacc_sem,
):
    patches, seqs, reqs, layers, slot, band, text_dev = dims
    peers = patches * reqs
    msg = layers * slot
    total_rows = layers * band
    patch, seq, req = (lax.axis_index(n) for n in ("patch", "seq", "req"))
    me = patch * reqs + req
    scale = 1.0 / math.sqrt(HEAD_DIM)
    n_chunks = len(CHUNKS)

    def peer(step):
        other = lax.rem(me + step, peers)
        return other, {"patch": other // reqs, "req": lax.rem(other, reqs)}

    loads = [
        pltpu.make_async_copy(src, dst, in_sems.at[i])
        for i, (src, dst) in enumerate(
            (
                (pm_hbm, pm_ref),
                (pos_hbm, pos_ref),
                (rows_hbm, rows_ref),
                (query_hbm, query_ref),
                (text_hbm, text_ref),
            )
        )
    ]
    loads[0].start()
    loads[1].start()
    loads[2].start()

    barrier = pltpu.get_barrier_semaphore()

    def greet(step, carry):
        _, device = peer(step)
        pl.semaphore_signal(barrier, inc=1, device_id=device, device_id_type=MESH)
        return carry

    lax.fori_loop(1, peers, greet, 0)
    for step in range(1, seqs):
        pl.semaphore_signal(
            barrier, inc=1, device_id={"seq": lax.rem(seq + step, seqs)}, device_id_type=MESH
        )
    loads[3].start()
    loads[4].start()

    loads[0].wait()
    loads[1].wait()
    owner = pm_ref[...]
    member = lax.broadcasted_iota(jnp.int32, (peers, band), 0) == owner
    member_f = member.astype(F32)
    before = lax.broadcasted_iota(jnp.int32, (band, band), 0) < lax.broadcasted_iota(
        jnp.int32, (band, band), 1
    )
    counts = jnp.dot(
        member_f.astype(BF16), before.astype(F32).astype(BF16), preferred_element_type=F32
    )
    rank = jnp.sum(member_f * counts, axis=0, keepdims=True)
    target = owner.astype(F32) * msg + rank
    line = lax.broadcasted_iota(jnp.int32, (total_rows, band), 0).astype(F32)
    for l in range(layers):
        sort_ref[:, l * band : (l + 1) * band] = (
            (line == target + float(l * slot)).astype(F32).astype(BF16)
        )

    local = pos_ref[...].astype(F32) - (seq * band).astype(F32)
    lane = lax.broadcasted_iota(jnp.int32, (peers, 128), 1)
    spread = ((lane // slot) % layers * band).astype(F32)
    for k in range(slot):
        mine = jnp.where(member & (counts == float(k)), local, 0.0)
        spread = spread + jnp.where(lane % slot == k, jnp.sum(mine, axis=1, keepdims=True), 0.0)
    place_send[...] = spread.reshape(peers, 1, 128)

    loads[2].wait()

    def sort_chunk(c):
        start, width = CHUNKS[c]
        for j in range(start, start + width, 256):
            def rows_of(i, carry):
                lines = pl.ds(pl.multiple_of(i * 256, 256), 256)
                send_ref[lines, j : j + 256] = jnp.dot(
                    sort_ref[lines, :], rows_ref[:, j : j + 256], preferred_element_type=F32
                ).astype(BF16)
                return carry
            lax.fori_loop(0, total_rows // 256, rows_of, 0)

    def block(ref, index, c):
        start, width = CHUNKS[c]
        return ref.at[pl.ds(pl.multiple_of(index * msg, msg), msg), pl.ds(start, width)]

    def send_chunk(c):
        def send(step, carry):
            other, device = peer(step)
            pltpu.make_async_remote_copy(
                src_ref=block(send_ref, other, c),
                dst_ref=block(got_ref, me, c),
                send_sem=send_sem,
                recv_sem=recv_sems.at[c],
                device_id=device,
                device_id_type=MESH,
            ).start()
            return carry
        lax.fori_loop(1, peers, send, 0)

    sort_chunk(0)
    pl.semaphore_wait(barrier, peers - 1 + seqs - 1)

    def send_place(step, carry):
        other, device = peer(step)
        pltpu.make_async_remote_copy(
            src_ref=place_send.at[other],
            dst_ref=place_got.at[me],
            send_sem=send_sem,
            recv_sem=place_sem,
            device_id=device,
            device_id_type=MESH,
        ).start()
        return carry

    lax.fori_loop(1, peers, send_place, 0)
    send_chunk(0)
    for c in range(1, n_chunks):
        sort_chunk(c)
        send_chunk(c)
    own = pl.ds(pl.multiple_of(me * msg, msg), msg)
    got_ref[own, :] = send_ref[own, :]
    place_got[pl.ds(me, 1)] = place_send[pl.ds(me, 1)]

    loads[3].wait()
    q_ref[...] = jnp.zeros_like(q_ref)
    for l in range(layers):
        whole = query_ref[l : l + 1, :].astype(F32)
        for h in range(HEADS):
            g, k = divmod(h, GROUP)
            q_ref[g, l * PAD + k : l * PAD + k + 1, :] = whole[:, h * HEAD_DIM : (h + 1) * HEAD_DIM]

    loads[4].wait()
    length = len_ref[0]
    text_at = lax.broadcasted_iota(jnp.int32, (PAD, text_dev), 1) + seq * text_dev
    used = text_at < length

    def dot_t(a, b):
        return lax.dot_general(a, b, (((1,), (1,)), ((), ())), preferred_element_type=F32)

    for g in range(KV_HEADS):
        keys = slice(g * HEAD_DIM, (g + 1) * HEAD_DIM)
        for l in range(layers):
            lines = slice(l * PAD, (l + 1) * PAD)
            raw = dot_t(q_ref[g, lines, :].astype(BF16), text_ref[l, :, keys]) * scale
            score_ref[g, lines, :] = jnp.where(used, raw, -jnp.inf)

    def wait_all(sem, ref):
        pltpu.make_async_copy(ref, ref, sem).wait()

    wait_all(place_sem, place_got.at[pl.ds(0, peers - 1)])
    per_tile = 128 // msg
    first = lax.broadcasted_iota(jnp.int32, (per_tile, 128), 0)
    which = lax.broadcasted_iota(jnp.int32, (per_tile, 128), 1) // msg
    cache_line = lax.broadcasted_iota(jnp.int32, (total_rows, 128), 0).astype(F32)
    for b in range(peers // per_tile):
        tile = place_got[b * per_tile : (b + 1) * per_tile].reshape(per_tile, 128)
        to = jnp.sum(jnp.where(first == which, tile, 0.0), axis=0, keepdims=True)
        place_ref[:, b * 128 : (b + 1) * 128] = (cache_line == to).astype(F32).astype(BF16)

    def place_chunk(c):
        start, width = CHUNKS[c]
        for j in range(start, start + width, 256):
            def rows_of(i, carry):
                lines = pl.ds(pl.multiple_of(i * 256, 256), 256)
                cache_ref[lines, j : j + 256] = jnp.dot(
                    place_ref[lines, :], got_ref[:, j : j + 256], preferred_element_type=F32
                ).astype(BF16)
                return carry
            lax.fori_loop(0, total_rows // 256, rows_of, 0)

    def wait_chunk(c):
        start, width = CHUNKS[c]
        wait_all(
            recv_sems.at[c], got_ref.at[pl.ds(0, (peers - 1) * msg), pl.ds(start, width)]
        )

    def exchange(src_ref, dst_ref, g, sem):
        @pl.when(seq != g)
        def _():
            pltpu.make_async_remote_copy(
                src_ref=src_ref.at[g],
                dst_ref=dst_ref.at[seq],
                send_sem=xsend_sem,
                recv_sem=sem,
                device_id={"seq": g},
                device_id_type=MESH,
            ).start()

    wait_chunk(0)
    same_layer = (
        lax.broadcasted_iota(jnp.int32, (layers * PAD, total_rows), 1) // slot
    ) % layers == lax.broadcasted_iota(jnp.int32, (layers * PAD, total_rows), 0) // PAD
    half = lax.broadcasted_iota(jnp.int32, (layers * PAD, 128), 1) < 64
    for g in range(KV_HEADS):
        keys = slice(g * HEAD_DIM, (g + 1) * HEAD_DIM)
        vals = slice((KV_HEADS + g) * HEAD_DIM, (KV_HEADS + g + 1) * HEAD_DIM)
        raw = dot_t(q_ref[g].astype(BF16), got_ref[:, keys]) * scale
        image = jnp.where(same_layer, raw, -jnp.inf)
        text = score_ref[g]
        top = jnp.maximum(
            jnp.max(image, axis=1, keepdims=True), jnp.max(text, axis=1, keepdims=True)
        )
        image_w = jnp.exp(image - top)
        text_w = jnp.exp(text - top)
        total = jnp.sum(image_w, axis=1, keepdims=True) + jnp.sum(text_w, axis=1, keepdims=True)
        weight_ref[g] = image_w.astype(BF16)
        stat_ref[g] = jnp.where(half, top, total)
        for l in range(layers):
            lines = slice(l * PAD, (l + 1) * PAD)
            acc_ref[g, lines, :] = jnp.dot(
                text_w[lines].astype(BF16), text_ref[l, :, vals], preferred_element_type=F32
            )
    for g in range(KV_HEADS):
        exchange(stat_ref, stat_got, g, xstat_sem)
    stat_got[pl.ds(seq, 1)] = stat_ref[pl.ds(seq, 1)]
    place_chunk(0)

    for c in range(1, n_chunks):
        wait_chunk(c)
        start, width = CHUNKS[c]
        heads = range(start // HEAD_DIM - KV_HEADS, (start + width) // HEAD_DIM - KV_HEADS)
        for g in heads:
            vals = slice((KV_HEADS + g) * HEAD_DIM, (KV_HEADS + g + 1) * HEAD_DIM)
            acc_ref[g] = acc_ref[g] + jnp.dot(
                weight_ref[g], got_ref[:, vals], preferred_element_type=F32
            )
        for g in heads:
            exchange(acc_ref, acc_got, g, xacc_sem)
        place_chunk(c)
    acc_got[pl.ds(seq, 1)] = acc_ref[pl.ds(seq, 1)]

    wait_all(xstat_sem, stat_got.at[pl.ds(0, seqs - 1)])
    tops = [stat_got[b][:, 0:1] for b in range(seqs)]
    totals = [stat_got[b][:, 64:65] for b in range(seqs)]
    top = functools.reduce(jnp.maximum, tops)
    factors = [jnp.exp(t - top) for t in tops]
    total = sum(f * t for f, t in zip(factors, totals))
    wait_all(xacc_sem, acc_got.at[pl.ds(0, seqs - 1)])
    summed = sum(f * acc_got[b] for b, f in enumerate(factors))
    result = summed / total
    for l in range(layers):
        for k in range(GROUP):
            att_ref[l : l + 1, k * HEAD_DIM : (k + 1) * HEAD_DIM] = result[
                l * PAD + k : l * PAD + k + 1, :
            ].astype(BF16)

    for c in range(n_chunks):
        start, width = CHUNKS[c]
        wait_all(send_sem, got_ref.at[pl.ds(0, (peers - 1) * msg), pl.ds(start, width)])
    wait_all(send_sem, place_got.at[pl.ds(0, peers - 1)])
    wait_all(xsend_sem, stat_got.at[pl.ds(0, seqs - 1)])
    wait_all(xsend_sem, acc_got.at[pl.ds(0, seqs - 1)])


def body(query, text_cache, text_len, image_rows, patch_map, image_places):
    layers = query.shape[0]
    text_dev = text_cache.shape[2]
    width = text_cache.shape[3]
    band = image_rows.shape[1]
    patches, seqs, reqs = (lax.axis_size(n) for n in ("patch", "seq", "req"))
    peers = patches * reqs
    slot = band // peers
    rows = layers * band
    heads = layers * PAD
    dims = (patches, seqs, reqs, layers, slot, band, text_dev)
    hbm = pl.BlockSpec(memory_space=pltpu.HBM)
    vmem = pl.BlockSpec(memory_space=pltpu.VMEM)
    attended, cache = pl.pallas_call(
        functools.partial(kernel, dims),
        name="reshard_attend",
        out_shape=(
            jax.ShapeDtypeStruct((layers, GROUP * HEAD_DIM), BF16),
            jax.ShapeDtypeStruct((rows, width), BF16),
        ),
        in_specs=[pl.BlockSpec(memory_space=pltpu.SMEM)] + [hbm] * 5,
        out_specs=(vmem, vmem),
        scratch_shapes=[
            pltpu.VMEM((1, band), jnp.int32),
            pltpu.VMEM((1, band), jnp.int32),
            pltpu.VMEM((layers, HEADS * HEAD_DIM), BF16),
            pltpu.VMEM((layers, text_dev, width), BF16),
            pltpu.VMEM((rows, width), BF16),
            pltpu.VMEM((rows, rows), BF16),
            pltpu.VMEM((rows, width), BF16),
            pltpu.VMEM((rows, width), BF16),
            pltpu.VMEM((rows, rows), BF16),
            pltpu.VMEM((peers, 1, 128), F32),
            pltpu.VMEM((peers, 1, 128), F32),
            pltpu.VMEM((KV_HEADS, heads, HEAD_DIM), F32),
            pltpu.VMEM((KV_HEADS, heads, text_dev), F32),
            pltpu.VMEM((KV_HEADS, heads, rows), BF16),
            pltpu.VMEM((KV_HEADS, heads, HEAD_DIM), F32),
            pltpu.VMEM((KV_HEADS, heads, HEAD_DIM), F32),
            pltpu.VMEM((seqs, heads, HEAD_DIM), F32),
            pltpu.VMEM((seqs, heads, HEAD_DIM), F32),
            pltpu.SemaphoreType.DMA((5,)),
            pltpu.SemaphoreType.DMA,
            pltpu.SemaphoreType.DMA((len(CHUNKS),)),
            pltpu.SemaphoreType.DMA,
            pltpu.SemaphoreType.DMA,
            pltpu.SemaphoreType.DMA,
            pltpu.SemaphoreType.DMA,
        ],
        compiler_params=pltpu.CompilerParams(
            collective_id=0, has_side_effects=True, vmem_limit_bytes=48 * 1024 * 1024
        ),
    )(
        text_len,
        *(
            pltpu.with_memory_space_constraint(x, pltpu.HBM)
            for x in (
                patch_map.reshape(1, band),
                image_places.reshape(1, band),
                query.reshape(layers, HEADS * HEAD_DIM),
                text_cache.reshape(layers, text_dev, width),
                image_rows.reshape(rows, width),
            )
        ),
    )
    return attended.reshape(layers, 1, GROUP * HEAD_DIM), cache.reshape(layers, 1, band, width)


def solution(mesh):
    return jax.shard_map(
        body,
        mesh=mesh,
        in_specs=(
            P(None, ("patch", "req"), None),
            P(None, ("patch", "req"), "seq", None),
            P(("patch", "req")),
            P(None, ("patch", "seq", "req"), None),
            P(("patch", "seq", "req")),
            P(("patch", "seq", "req")),
        ),
        out_specs=(P(None, ("patch", "req"), "seq"), P(None, ("patch", "req"), "seq", None)),
        check_vma=False,
    )
```

```python
import functools
import math

import jax
import jax.numpy as jnp
from jax import lax
from jax.experimental import pallas as pl
from jax.experimental.pallas import tpu as pltpu
from jax.sharding import PartitionSpec as P

HEADS = 28
KV_HEADS = 4
HEAD_DIM = 128
GROUP = HEADS // KV_HEADS
KVW = KV_HEADS * HEAD_DIM
PAD = 8
MESH = pl.DeviceIdType.MESH
BF16 = jnp.bfloat16
F32 = jnp.float32
CHUNKS = ((0, 256), (256, 256), (512, 384), (896, 128))
LAST = len(CHUNKS) - 1
TILE = 256


def lanes(index):
    return pl.ds(pl.multiple_of(index * HEAD_DIM, HEAD_DIM), HEAD_DIM)


def loop(start, stop, step):
    def run(i, carry):
        step(i)
        return carry

    lax.fori_loop(start, stop, run, 0)


def reshard_kernel(
    dims,
    len_ref, pm_hbm, pos_hbm, query_hbm, text_hbm, rows_hbm,
    place_ref, cache_ref, last_ref, own_w_ref, merge_ref,
    pm_ref, pos_ref, query_ref, text_ref, rows_ref,
    sort_ref, send_ref, got_ref, place_send, place_got,
    q_ref, score_ref, weight_ref, acc_ref, stat_ref, acc_got, stat_got,
    in_sems, send_sem, recv_sems, place_sem, xsend_sem, xstat_sem, xacc_sem,
):
    patches, seqs, reqs, layers, slot, band, text_dev = dims
    peers = patches * reqs
    msg = layers * slot
    total_rows = layers * band
    heads = layers * PAD
    patch, seq, req = (lax.axis_index(n) for n in ("patch", "seq", "req"))
    me = patch * reqs + req
    scale = 1.0 / math.sqrt(HEAD_DIM)

    def peer(step):
        other = me + step
        other = jnp.where(other >= peers, other - peers, other)
        return other, {"patch": other // reqs, "req": lax.rem(other, reqs)}

    def head_at(j):
        return lax.rem(seq + 1 + j, seqs)

    loads = [
        pltpu.make_async_copy(src, dst, in_sems.at[i])
        for i, (src, dst) in enumerate(
            (
                (pm_hbm, pm_ref),
                (rows_hbm, rows_ref),
                (pos_hbm, pos_ref),
                (query_hbm, query_ref),
                (text_hbm, text_ref),
            )
        )
    ]
    for i in range(3):
        loads[i].start()

    barrier = pltpu.get_barrier_semaphore()

    def greet(i):
        step = i + peers // 4
        _, device = peer(jnp.where(step >= peers, step - peers + 1, step))
        pl.semaphore_signal(barrier, inc=1, device_id=device, device_id_type=MESH)

    loop(0, peers - 1, greet)
    for step in range(1, seqs):
        pl.semaphore_signal(
            barrier, inc=1, device_id={"seq": lax.rem(seq + step, seqs)}, device_id_type=MESH
        )

    loads[0].wait()
    owner = pm_ref[...]
    member = lax.broadcasted_iota(jnp.int32, (peers, band), 0) == owner
    member_f = member.astype(F32)
    before = lax.broadcasted_iota(jnp.int32, (band, band), 0) < lax.broadcasted_iota(
        jnp.int32, (band, band), 1
    )
    counts = jnp.dot(
        member_f.astype(BF16), before.astype(F32).astype(BF16), preferred_element_type=F32
    )
    rank = jnp.sum(member_f * counts, axis=0, keepdims=True)
    target = owner.astype(F32) * msg + rank
    line = lax.broadcasted_iota(jnp.int32, (total_rows, band), 0).astype(F32)
    for l in range(layers):
        sort_ref[:, l * band : (l + 1) * band] = (
            (line == target + float(l * slot)).astype(F32).astype(BF16)
        )

    def sort_columns(source, start, width):
        def rows_of(i):
            lines = pl.ds(pl.multiple_of(i * TILE, TILE), TILE)
            send_ref[lines, start : start + width] = jnp.dot(
                sort_ref[lines, :], rows_ref[:, source], preferred_element_type=F32
            ).astype(BF16)

        loop(0, total_rows // TILE, rows_of)

    def sort_chunk(c):
        start, width = CHUNKS[c]
        if start < KVW:
            for j in range(start, start + width, TILE):
                sort_columns(slice(j, j + TILE), j, TILE)
        else:
            for j in range(start, start + width, HEAD_DIM):
                sort_columns(lanes(KV_HEADS + head_at((j - KVW) // HEAD_DIM)), j, HEAD_DIM)

    def arrivals(c):
        start, width = CHUNKS[c]
        return (last_ref, 0, width) if c == LAST else (got_ref, start, width)

    def block(ref, index, start, width):
        return ref.at[pl.ds(pl.multiple_of(index * msg, msg), msg), pl.ds(start, width)]

    def send_chunk(c):
        def send(step):
            other, device = peer(step)
            pltpu.make_async_remote_copy(
                src_ref=block(send_ref, other, *CHUNKS[c]),
                dst_ref=block(arrivals(c)[0], me, *arrivals(c)[1:]),
                send_sem=send_sem,
                recv_sem=recv_sems.at[c],
                device_id=device,
                device_id_type=MESH,
            ).start()

        loop(1, peers, send)

    loads[1].wait()
    sort_chunk(0)
    pl.semaphore_wait(barrier, peers - 1 + seqs - 1)
    send_chunk(0)
    loads[3].start()
    loads[4].start()

    loads[2].wait()
    local = pos_ref[...].astype(F32) - (seq * band).astype(F32)
    lane = lax.broadcasted_iota(jnp.int32, (peers, 128), 1)
    spread = ((lane // slot) % layers * band).astype(F32)
    for k in range(slot):
        mine = jnp.where(member & (counts == float(k)), local, 0.0)
        spread = spread + jnp.where(lane % slot == k, jnp.sum(mine, axis=1, keepdims=True), 0.0)
    place_send[...] = spread.reshape(peers, 1, 128)

    for c in range(1, LAST + 1):
        sort_chunk(c)
        send_chunk(c)
        if c == 1:

            def send_place(step):
                other, device = peer(step)
                pltpu.make_async_remote_copy(
                    src_ref=place_send.at[other],
                    dst_ref=place_got.at[me],
                    send_sem=send_sem,
                    recv_sem=place_sem,
                    device_id=device,
                    device_id_type=MESH,
                ).start()

            loop(1, peers, send_place)
    own = pl.ds(pl.multiple_of(me * msg, msg), msg)
    got_ref[own, :] = send_ref[own, : CHUNKS[LAST][0]]
    last_ref[own, :] = send_ref[own, CHUNKS[LAST][0] :]
    place_got[pl.ds(me, 1)] = place_send[pl.ds(me, 1)]

    loads[3].wait()
    q_ref[...] = jnp.zeros_like(q_ref)
    for l in range(layers):
        whole = query_ref[l : l + 1, :].astype(F32)
        for h in range(HEADS):
            g, k = divmod(h, GROUP)
            q_ref[g, l * PAD + k : l * PAD + k + 1, :] = whole[:, h * HEAD_DIM : (h + 1) * HEAD_DIM]

    loads[4].wait()
    length = len_ref[0]
    text_at = lax.broadcasted_iota(jnp.int32, (PAD, text_dev), 1) + seq * text_dev
    used = text_at < length

    def dot_t(a, b):
        return lax.dot_general(a, b, (((1,), (1,)), ((), ())), preferred_element_type=F32)

    for g in range(KV_HEADS):
        keys = slice(g * HEAD_DIM, (g + 1) * HEAD_DIM)
        for l in range(layers):
            lines = slice(l * PAD, (l + 1) * PAD)
            raw = dot_t(q_ref[g, lines, :].astype(BF16), text_ref[l, :, keys]) * scale
            score_ref[g, lines, :] = jnp.where(used, raw, -jnp.inf)

    def wait_all(sem, ref):
        pltpu.make_async_copy(ref, ref, sem).wait()

    def wait_chunk(c):
        ref, start, width = arrivals(c)
        wait_all(recv_sems.at[c], ref.at[pl.ds(0, (peers - 1) * msg), pl.ds(start, width)])

    wait_all(place_sem, place_got.at[pl.ds(0, peers - 1)])
    per_tile = 128 // msg
    first = lax.broadcasted_iota(jnp.int32, (per_tile, 128), 0)
    which = lax.broadcasted_iota(jnp.int32, (per_tile, 128), 1) // msg
    cache_line = lax.broadcasted_iota(jnp.int32, (total_rows, 128), 0).astype(F32)
    for b in range(peers // per_tile):
        tile = place_got[b * per_tile : (b + 1) * per_tile].reshape(per_tile, 128)
        to = jnp.sum(jnp.where(first == which, tile, 0.0), axis=0, keepdims=True)
        place_ref[:, b * 128 : (b + 1) * 128] = (cache_line == to).astype(F32).astype(BF16)

    def place_columns(start, width, to):
        def rows_of(i):
            lines = pl.ds(pl.multiple_of(i * TILE, TILE), TILE)
            cache_ref[lines, to] = jnp.dot(
                place_ref[lines, :], got_ref[:, start : start + width], preferred_element_type=F32
            ).astype(BF16)

        loop(0, total_rows // TILE, rows_of)

    def exchange(src_ref, dst_ref, j, sem):
        pltpu.make_async_remote_copy(
            src_ref=src_ref.at[head_at(j)],
            dst_ref=dst_ref.at[j],
            send_sem=xsend_sem,
            recv_sem=sem,
            device_id={"seq": head_at(j)},
            device_id_type=MESH,
        ).start()

    for c in (0, 1):
        wait_chunk(c)
    same_layer = (
        lax.broadcasted_iota(jnp.int32, (heads, total_rows), 1) // slot
    ) % layers == lax.broadcasted_iota(jnp.int32, (heads, total_rows), 0) // PAD
    half = lax.broadcasted_iota(jnp.int32, (heads, 128), 1) < 64
    for g in range(KV_HEADS):
        keys = slice(g * HEAD_DIM, (g + 1) * HEAD_DIM)
        vals = slice(KVW + g * HEAD_DIM, KVW + (g + 1) * HEAD_DIM)
        raw = dot_t(q_ref[g].astype(BF16), got_ref[:, keys]) * scale
        image = jnp.where(same_layer, raw, -jnp.inf)
        text = score_ref[g]
        top = jnp.maximum(
            jnp.max(image, axis=1, keepdims=True), jnp.max(text, axis=1, keepdims=True)
        )
        image_w = jnp.exp(image - top)
        text_w = jnp.exp(text - top)
        total = jnp.sum(image_w, axis=1, keepdims=True) + jnp.sum(text_w, axis=1, keepdims=True)
        weight_ref[g] = image_w.astype(BF16)
        stat_ref[g] = jnp.where(half, top, total)
        for l in range(layers):
            lines = slice(l * PAD, (l + 1) * PAD)
            acc_ref[g, lines, :] = jnp.dot(
                text_w[lines].astype(BF16), text_ref[l, :, vals], preferred_element_type=F32
            )
    for j in range(seqs - 1):
        exchange(stat_ref, stat_got, j, xstat_sem)
    own_w_ref[...] = weight_ref[seq]
    for j in range(0, KVW, TILE):
        place_columns(j, TILE, slice(j, j + TILE))

    wait_chunk(2)
    for j in range(seqs - 1):
        g = head_at(j)
        start = KVW + j * HEAD_DIM
        acc_ref[g] = acc_ref[g] + jnp.dot(
            weight_ref[g], got_ref[:, start : start + HEAD_DIM], preferred_element_type=F32
        )
    for j in range(seqs - 1):
        exchange(acc_ref, acc_got, j, xacc_sem)
    for j in range(seqs - 1):
        place_columns(KVW + j * HEAD_DIM, HEAD_DIM, lanes(KV_HEADS + head_at(j)))

    wait_all(xstat_sem, stat_got)
    stats = [stat_ref[seq]] + [stat_got[j] for j in range(seqs - 1)]
    top = functools.reduce(jnp.maximum, [s[:, 0:1] for s in stats])
    factors = [jnp.exp(s[:, 0:1] - top) for s in stats]
    total = sum(f * s[:, 64:65] for f, s in zip(factors, stats))
    wait_all(xacc_sem, acc_got)
    merge_ref[0] = factors[0] * acc_ref[seq] + sum(
        f * acc_got[j] for j, f in enumerate(factors[1:])
    )
    merge_ref[1] = jnp.broadcast_to(factors[0], (heads, HEAD_DIM))
    merge_ref[2] = jnp.broadcast_to(total, (heads, HEAD_DIM))

    for c in range(LAST):
        wait_all(
            send_sem, got_ref.at[pl.ds(0, (peers - 1) * msg), pl.ds(CHUNKS[c][0], CHUNKS[c][1])]
        )
    wait_all(send_sem, place_got.at[pl.ds(0, peers - 1)])
    wait_all(xsend_sem, stat_got)
    wait_all(xsend_sem, acc_got)
    wait_all(send_sem, last_ref.at[pl.ds(0, (peers - 1) * msg)])
    wait_chunk(LAST)


def finish_kernel(
    dims,
    place_ref, cache_ref, last_ref, own_w_ref, merge_ref,
    att_hbm, cache_hbm,
    att_ref, part_ref, sems,
):
    _, seqs, _, layers, _, band, _ = dims
    total_rows = layers * band
    seq = lax.axis_index("seq")
    copies = [pltpu.make_async_copy(cache_ref.at[:, :KVW], cache_hbm.at[:, :KVW], sems.at[0])]
    for j in range(seqs - 1):
        columns = lanes(KV_HEADS + lax.rem(seq + 1 + j, seqs))
        copies.append(
            pltpu.make_async_copy(
                cache_ref.at[:, columns], cache_hbm.at[:, columns], sems.at[1 + j]
            )
        )
    for copy in copies:
        copy.start()

    values = jnp.dot(own_w_ref[...], last_ref[...], preferred_element_type=F32)
    result = (merge_ref[0] + merge_ref[1] * values) / merge_ref[2]
    for l in range(layers):
        for k in range(GROUP):
            att_ref[l : l + 1, k * HEAD_DIM : (k + 1) * HEAD_DIM] = result[
                l * PAD + k : l * PAD + k + 1, :
            ].astype(BF16)
    copies.append(pltpu.make_async_copy(att_ref, att_hbm, sems.at[seqs]))
    copies[-1].start()

    columns = lanes(KV_HEADS + seq)
    for i in range(total_rows // TILE):
        lines = slice(i * TILE, (i + 1) * TILE)
        part_ref[lines, :] = jnp.dot(
            place_ref[lines, :], last_ref[...], preferred_element_type=F32
        ).astype(BF16)
        copies.append(
            pltpu.make_async_copy(
                part_ref.at[lines, :], cache_hbm.at[lines, columns], sems.at[seqs + 1 + i]
            )
        )
        copies[-1].start()
    for copy in copies:
        copy.wait()


def body(query, text_cache, text_len, image_rows, patch_map, image_places):
    layers = query.shape[0]
    text_dev = text_cache.shape[2]
    width = text_cache.shape[3]
    band = image_rows.shape[1]
    patches, seqs, reqs = (lax.axis_size(n) for n in ("patch", "seq", "req"))
    peers = patches * reqs
    slot = band // peers
    rows = layers * band
    heads = layers * PAD
    dims = (patches, seqs, reqs, layers, slot, band, text_dev)
    hbm = pl.BlockSpec(memory_space=pltpu.HBM)
    vmem = pl.BlockSpec(memory_space=pltpu.VMEM)
    parts = pl.pallas_call(
        functools.partial(reshard_kernel, dims),
        name="reshard",
        out_shape=(
            jax.ShapeDtypeStruct((rows, rows), BF16),
            jax.ShapeDtypeStruct((rows, width), BF16),
            jax.ShapeDtypeStruct((rows, HEAD_DIM), BF16),
            jax.ShapeDtypeStruct((heads, rows), BF16),
            jax.ShapeDtypeStruct((3, heads, HEAD_DIM), F32),
        ),
        in_specs=[pl.BlockSpec(memory_space=pltpu.SMEM)] + [hbm] * 5,
        out_specs=(vmem,) * 5,
        scratch_shapes=[
            pltpu.VMEM((1, band), jnp.int32),
            pltpu.VMEM((1, band), jnp.int32),
            pltpu.VMEM((layers, HEADS * HEAD_DIM), BF16),
            pltpu.VMEM((layers, text_dev, width), BF16),
            pltpu.VMEM((rows, width), BF16),
            pltpu.VMEM((rows, rows), BF16),
            pltpu.VMEM((rows, width), BF16),
            pltpu.VMEM((rows, width - HEAD_DIM), BF16),
            pltpu.VMEM((peers, 1, 128), F32),
            pltpu.VMEM((peers, 1, 128), F32),
            pltpu.VMEM((KV_HEADS, heads, HEAD_DIM), F32),
            pltpu.VMEM((KV_HEADS, heads, text_dev), F32),
            pltpu.VMEM((KV_HEADS, heads, rows), BF16),
            pltpu.VMEM((KV_HEADS, heads, HEAD_DIM), F32),
            pltpu.VMEM((KV_HEADS, heads, HEAD_DIM), F32),
            pltpu.VMEM((seqs - 1, heads, HEAD_DIM), F32),
            pltpu.VMEM((seqs - 1, heads, HEAD_DIM), F32),
            pltpu.SemaphoreType.DMA((5,)),
            pltpu.SemaphoreType.DMA,
            pltpu.SemaphoreType.DMA((len(CHUNKS),)),
            pltpu.SemaphoreType.DMA,
            pltpu.SemaphoreType.DMA,
            pltpu.SemaphoreType.DMA,
            pltpu.SemaphoreType.DMA,
        ],
        compiler_params=pltpu.CompilerParams(
            collective_id=0, has_side_effects=True, vmem_limit_bytes=48 * 1024 * 1024
        ),
    )(
        text_len,
        *(
            pltpu.with_memory_space_constraint(x, pltpu.HBM)
            for x in (
                patch_map.reshape(1, band),
                image_places.reshape(1, band),
                query.reshape(layers, HEADS * HEAD_DIM),
                text_cache.reshape(layers, text_dev, width),
                image_rows.reshape(rows, width),
            )
        ),
    )
    attended, cache = pl.pallas_call(
        functools.partial(finish_kernel, dims),
        name="finish",
        out_shape=(
            jax.ShapeDtypeStruct((layers, GROUP * HEAD_DIM), BF16),
            jax.ShapeDtypeStruct((rows, width), BF16),
        ),
        in_specs=[vmem] * 5,
        out_specs=(hbm, hbm),
        scratch_shapes=[
            pltpu.VMEM((layers, GROUP * HEAD_DIM), BF16),
            pltpu.VMEM((rows, HEAD_DIM), BF16),
            pltpu.SemaphoreType.DMA((seqs + 1 + rows // TILE,)),
        ],
        compiler_params=pltpu.CompilerParams(vmem_limit_bytes=16 * 1024 * 1024),
    )(*parts)
    return (
        attended.reshape(layers, 1, GROUP * HEAD_DIM),
        cache.reshape(layers, 1, band, width),
    )


def solution(mesh):
    return jax.shard_map(
        body,
        mesh=mesh,
        in_specs=(
            P(None, ("patch", "req"), None),
            P(None, ("patch", "req"), "seq", None),
            P(("patch", "req")),
            P(None, ("patch", "seq", "req"), None),
            P(("patch", "seq", "req")),
            P(("patch", "seq", "req")),
        ),
        out_specs=(P(None, ("patch", "req"), "seq"), P(None, ("patch", "req"), "seq", None)),
        check_vma=False,
    )
```
